32 devices in a mesh: ga: 1, ea: 32 (over z, y, x, core).
Axes of the slice: x: 2, y: 2, z: 4, core: 2. Of those that a mesh axis runs over, the one named last changes fastest.
Arguments:
- tokens: bfloat16 [256, 7168], P(('ga', 'ea')), may hold values from -6 to 6
- route_slot: int32 [256, 2], P(('ga', 'ea')), may hold values from 0 to 3, all different within a row; in each aligned block of 8 rows (0 to 7, 8 to 15, ...) at most 8 rows name the same one
- gates: float32 [256, 2], P(('ga', 'ea')), may hold values from 0.2 to 1
- gate_up: bfloat16 [32, 7168, 512], P('ea'), may hold values from -0.0625 to 0.0625
- down: bfloat16 [32, 256, 7168], P('ea'), may hold values from -0.125 to 0.125
Outputs:
- mixed: bfloat16 [256, 7168], P(('ga', 'ea'))
The draws below stay inside these ranges and needn't reach their ends.
Inputs may be any that keep to these rules, and one draw needn't show every extreme that they name: `route_slot`: each token names 2 different replicas. Among the tokens of one device no replica is named more than 8 times, and some device names some replica exactly 8 times.
All inputs are finite; a program needn't handle non-finite values.
Results may differ from the reference program's by a relative error of at most 0.0087.
Values may be sent and summed in bfloat16 or wider, within the bound.
A program may use at most 64 MiB of HBM per device.

```python
import math
import jax
import jax.numpy as jnp
import numpy as np
from jax import lax

D = 7168
FF = 2048
TP = 8
TOPK = 2
TOK_DEV = 8
HS = 256
SLOTS = 4
CAP = 8
TOKENS = 256
N_EA = 32


def levels(own_key, shape, cuts, smallest, high):
    loudness = 1.0
    for dim, shards_of in cuts:
        heights = jax.random.uniform(jax.random.fold_in(jax.random.fold_in(own_key, 6), dim), (shards_of,), jnp.float32, smallest / len(cuts), high / len(cuts))
        loudness = loudness * jnp.repeat(jnp.exp(heights), shape[dim] // shards_of).reshape((-1,) + (1,) * (len(shape) - 1 - dim))
    return loudness


def routed_block(own_key, own, number, rows, number_of, top, reach, slope):
    sequence = jax.random.permutation(own_key, number_of)
    crowded, ordinary = shares(number_of, rows * top, reach, slope, True), shares(number_of, rows * top, reach, slope, False)
    places = jnp.arange(number_of)

    def named(sizes, offset_by):
        used = int((sizes > 0).sum())
        fixed = max(1, used // 4)
        passed = fixed + (places - fixed + offset_by * (used - fixed)) % max(1, number_of - fixed)
        return jnp.zeros((number_of,), jnp.int32).at[sequence[jnp.where(places < fixed, places, passed)]].set(jnp.asarray(sizes, jnp.int32))

    sizes = jnp.where(number % 4 == 0, named(crowded, number // 4), named(ordinary, number - number // 4 - 1))
    mixed = jax.random.permutation(jax.random.fold_in(own, 3), number_of)
    donor, receiver = mixed[0:number_of // 2 * 2:2], mixed[1:number_of // 2 * 2:2]
    slack = jnp.minimum(sizes[donor] - 1, reach - sizes[receiver]) // 2
    slack = jnp.where((donor == sequence[0]) | (receiver == sequence[0]) | (sizes[receiver] == 0), 0, jnp.maximum(slack, 0))
    passed = jax.random.randint(jax.random.fold_in(own, 4), (number_of // 2,), 0, 1 << 20) % (slack + 1)
    sizes = sizes.at[donor].add(-passed).at[receiver].add(passed)
    items = jnp.searchsorted(jnp.cumsum(sizes), jnp.arange(rows * top), side="right").astype(jnp.int32)
    grid = items.reshape(top, rows).T
    grid = grid[jax.random.permutation(jax.random.fold_in(own, 1), rows)]
    offset_by = jax.random.randint(jax.random.fold_in(own, 2), (rows, 1), 0, top)
    return jnp.take_along_axis(grid, (jnp.arange(top)[None, :] + offset_by) % top, axis=1)


def shares(number_of, total, bound, slope, full):
    weights = [(1 << 20) // math.isqrt(standing ** slope) + 1 for standing in range(1, number_of + 1)]
    largest = bound if full else min(bound, max(-(-total // number_of), total * weights[0] // sum(weights)))
    least = 1 if total - largest >= number_of - 1 else 0
    given, surplus = [largest] + [least] * (number_of - 1), total - largest - least * (number_of - 1)
    while surplus > 0:
        candidates = [i for i in range(1, number_of) if given[i] < largest] or [i for i in range(1, number_of) if given[i] < bound]
        mass, left = sum([weights[i] for i in candidates]), surplus
        for i in candidates:
            more = min(bound - given[i], max(1, left * weights[i] // mass), surplus)
            given[i] = given[i] + more
            surplus = surplus - more
    return np.array(given)


def normal_values(rng, extent, spread, limit, cuts=(), held_as=jnp.bfloat16):
    loudness = levels(rng, extent, cuts, -0.22, 0.18) if cuts else 1.0
    values = jax.random.normal(rng, extent, jnp.float32) * spread * loudness
    return jnp.minimum(jnp.maximum(values, -limit), limit).astype(held_as)


def setup_inputs(seed: int = 0, part: int = 0) -> dict:
    key_of = jax.random.split(jax.random.key(seed), 6)
    part_splits = jax.random.split(jax.random.fold_in(key_of[5], part), 6)
    tokens = normal_values(part_splits[0], (TOKENS, D), 1.0, 6.0, ((0, 32),))
    route_slot_keys = jax.random.split(jax.random.fold_in(part_splits[1], 1), TOKENS // TOK_DEV)
    route_slot_turns = jax.random.permutation(jax.random.fold_in(part_splits[1], 3), TOKENS // TOK_DEV)
    route_slot = jax.vmap(lambda own, number: routed_block(jax.random.fold_in(part_splits[1], 2), own, number, TOK_DEV, SLOTS, TOPK, CAP, 2))(route_slot_keys, route_slot_turns).reshape((TOKENS, TOPK))
    gates = jnp.clip(0.2 + 0.8 * jax.random.uniform(part_splits[2], (TOKENS, TOPK), jnp.float32) ** levels(part_splits[2], (TOKENS, TOPK), ((0, 32),), -0.2, 0.2), 0.2, 1.0)
    gate_up = normal_values(key_of[3], (N_EA, D, 2 * HS), D ** -0.5, 0.0625, ((0, 32),))
    down = normal_values(key_of[4], (N_EA, HS, D), FF ** -0.5, 0.125, ((0, 32),))
    return {"tokens": tokens, "route_slot": route_slot, "gates": gates, "gate_up": gate_up, "down": down}


def reference(tokens, route_slot, gates, gate_up, down):
    pairs = TOKENS * TOPK
    flat_slot = route_slot.reshape(-1).astype(jnp.int32)
    flat_gate = gates.reshape(-1)
    owner = (jnp.arange(pairs, dtype=jnp.int32) // TOPK).astype(jnp.int32)
    order = jnp.argsort(flat_slot, stable=True).astype(jnp.int32)
    counts = jnp.sum((flat_slot[:, None] == jnp.arange(SLOTS, dtype=jnp.int32)[None, :]).astype(jnp.int32), axis=0)
    starts = (jnp.cumsum(counts) - counts).astype(jnp.int32)
    most_rows = N_EA * CAP

    def one_slot(total, slot):
        begin = jnp.minimum(starts[slot], pairs - most_rows).astype(jnp.int32)
        picked = lax.dynamic_slice_in_dim(order, begin, most_rows, 0)
        member = (flat_slot[picked] == slot)
        rows = tokens[owner[picked]]
        blocks = lax.dynamic_slice_in_dim(gate_up, (slot * TP).astype(jnp.int32), TP, 0)
        wide = jnp.transpose(blocks, (1, 0, 2)).reshape(D, TP * 2 * HS)
        both = jnp.dot(rows, wide, preferred_element_type=jnp.float32).reshape(most_rows, TP, 2 * HS)
        hidden = (jax.nn.silu(both[:, :, :HS]) * both[:, :, HS:]).astype(jnp.bfloat16).reshape(most_rows, FF)
        downs = lax.dynamic_slice_in_dim(down, (slot * TP).astype(jnp.int32), TP, 0).reshape(FF, D)
        result = jnp.dot(hidden, downs, preferred_element_type=jnp.float32)
        weight = jnp.where(member, flat_gate[picked], jnp.float32(0.0))
        total = total.at[owner[picked]].add(result * weight[:, None])
        return total, None

    total, unused = lax.scan(one_slot, jnp.zeros((TOKENS, D), jnp.float32), jnp.arange(SLOTS, dtype=jnp.int32))
    return total.astype(jnp.bfloat16)
```

```python
import functools

import jax
import jax.numpy as jnp
from jax import lax
from jax.experimental import pallas as pl
from jax.experimental.pallas import tpu as pltpu
from jax.sharding import PartitionSpec as P

TP = 8
LANES = 128
F32 = jnp.float32
BF16 = jnp.bfloat16


def copies_per_launch(outer):
    return 26 * outer + 8


def visits(place, outer):
    rest = [o for o in range(outer) if o // 2 != place // 2]
    return [place, place ^ 1] + sorted(rest, key=lambda o: abs(o - place))


def spans(begin, end, step):
    return [(at, min(step, end - at)) for at in range(begin, end, step)]


def column(row, count):
    down = lax.broadcasted_iota(jnp.int32, (count, count), 0)
    across = lax.broadcasted_iota(jnp.int32, (count, count), 1)
    return jnp.sum(jnp.where(down == across, row, 0.0), axis=1, keepdims=True)


def split(width):
    tiles = width // LANES
    cut = tiles // 2 * LANES
    quarter = cut + (tiles + 1 - tiles // 2) // 2 * LANES
    half = width // 2
    a = half // LANES // 2 * LANES
    g = a + (half - a) // LANES // 2 * LANES
    return cut, quarter, half, a, g


def kernel(outer, schedule, *refs):
    tokens, route, gates, gate_up, down, out = refs[:6]
    xin, acc, hid, hid_sib, weight, w_in, w_out = refs[6:13]
    a_part, b_part, c_part, d_part, f_in = refs[13:18]
    a_one, b_one, c_one, d_one = refs[18:22]
    a_mid, b_mid, c_mid, d_mid = refs[22:26]
    a_two, b_two, c_two, d_two = refs[26:30]
    z_send, z_recv, route_in, gates_in = refs[30:34]
    send_sems, recv_sems, w_sems = refs[34:]

    place = lax.axis_index("ea")
    plane = place // TP
    inner = place % TP
    core, x, y = inner % 2, inner // 2 % 2, inner // 4
    slots = {
        "own": core * 4 + y * 2 + x,
        "x": core * 4 + y * 2 + (1 - x),
        "y": core * 4 + (1 - y) * 2 + x,
        "d": core * 4 + (1 - y) * 2 + (1 - x),
    }
    base = plane * TP
    devs = {
        "c": base + y * 4 + x * 2 + (1 - core),
        "x": base + y * 4 + (1 - x) * 2 + core,
        "y": base + (1 - y) * 4 + x * 2 + core,
    }
    table = [visits(o, outer) for o in range(outer)]
    near = [plane]
    for i in range(1, outer):
        o = table[0][i] * jnp.int32(1)
        for p in range(1, outer):
            o = jnp.where(plane == p, table[p][i], o)
        near.append(o)
    mate = plane + 1 - 2 * (plane % 2)
    beyond = 2 * plane - mate
    has_beyond = (beyond >= 0) & (beyond < outer)
    mate_dev = mate * TP + inner
    beyond_dev = jnp.where(has_beyond, beyond, mate) * TP + inner

    def signal(dev):
        pl.semaphore_signal(
            barrier, inc=1, device_id={"ea": dev}, device_id_type=pl.DeviceIdType.MESH
        )

    barrier = pltpu.get_barrier_semaphore()
    for dev in (devs["c"], devs["x"], devs["y"], mate_dev):
        signal(dev)
    pl.when(has_beyond)(lambda: signal(beyond_dev))

    tok_rows, width = tokens.shape
    wide = width + LANES
    cut, quarter, half, a_cols, g_cols = split(width)
    chunk = [pl.ds(0, cut), pl.ds(cut, wide - cut)]
    small_chunk = [pl.ds(cut, quarter - cut), pl.ds(quarter, wide - quarter)]
    mine = xin.at[plane, slots["own"]]
    small = [
        pltpu.make_async_copy(tokens, mine.at[:, pl.ds(0, width)], w_sems.at[2]),
        pltpu.make_async_copy(route, route_in, w_sems.at[3]),
        pltpu.make_async_copy(gates, gates_in, w_sems.at[4]),
    ]
    for copy in small:
        copy.start()
    in_copy = pltpu.make_async_copy(gate_up.at[0], w_in, w_sems.at[0])
    in_copy.start()
    units = down.shape[1]
    my_half = pl.ds(pl.multiple_of(core * half, LANES), half)
    sib_half = pl.ds(pl.multiple_of((1 - core) * half, LANES), half)
    down_copy = pltpu.make_async_copy(
        down.at[0, :, my_half], w_out.at[pl.ds(0, units)], w_sems.at[1]
    )
    down_copy.start()
    rows = TP * tok_rows
    hidden_cols = w_in.shape[1] // 2

    small[1].wait()
    small[2].wait()
    lane = lax.broadcasted_iota(jnp.int32, (tok_rows, LANES), 1)
    gate = jnp.zeros((tok_rows, LANES), F32)
    for j in range(route.shape[0]):
        chosen = column(route_in[j : j + 1, :].astype(F32), tok_rows)
        value = column(gates_in[j : j + 1, :], tok_rows)
        gate = gate + jnp.where(chosen == (lane % outer).astype(F32), value, 0.0)
    high = gate.astype(BF16).astype(F32)
    mid = (gate - high).astype(BF16).astype(F32)
    low = gate - high - mid
    term = lane // outer
    terms = jnp.where(
        term == 0, high, jnp.where(term == 1, mid, jnp.where(term == 2, low, 0.0))
    )
    xin[plane, slots["own"], :, pl.ds(width, LANES)] = terms.astype(BF16)

    small[0].wait()
    pl.semaphore_wait(barrier, 4 + has_beyond.astype(jnp.int32))

    sent = []
    fixed = 4 * outer + 2 * outer

    def remote(src, dst, dev, arrival=None, when=None):
        copy = pltpu.make_async_remote_copy(
            src_ref=src,
            dst_ref=dst,
            send_sem=send_sems.at[len(sent)],
            recv_sem=recv_sems.at[fixed + len(sent) if arrival is None else arrival],
            device_id={"ea": dev},
            device_id_type=pl.DeviceIdType.MESH,
        )
        if when is None:
            copy.start()
        else:
            pl.when(when)(copy.start)
        sent.append((copy, when))
        return copy

    def arrived(ref, number):
        pltpu.make_async_remote_copy(
            src_ref=ref,
            dst_ref=ref,
            send_sem=send_sems.at[0],
            recv_sem=recv_sems.at[number],
            device_id={"ea": devs["c"]},
            device_id_type=pl.DeviceIdType.MESH,
        ).wait_recv()

    def gather_sem(o, h):
        return 2 * o + h

    def result_sem(o, c, h):
        return 2 * outer + 4 * o + 2 * c + h

    copies = {}
    to_core = {(i, h): [] for i in range(outer) for h in range(2)}

    def same(i, who, cols, dev):
        block = xin.at[near[i], slots[who], :, cols]
        return remote(block, block, devs[dev])

    def share(i, who, h, cols=None):
        to_core[i, h].append(same(i, who, chunk[h] if cols is None else cols, "c"))

    def up_to_mate(k, who):
        block = xin.at[plane, slots[who], :, chunk[0]]
        copies["m", k] = remote(block, block, mate_dev)

    def spread(i, h):
        o = near[i]
        block = xin.at[o, slots["own"], :, chunk[h]]
        number = gather_sem(o, h)
        if i == 0:
            remote(block, block, mate_dev, number)
            remote(block, block, beyond_dev, number, has_beyond)
        else:
            arrived(block, number)
            onward = jnp.where(o < plane, plane + 1, plane - 1)
            exists = (onward >= 0) & (onward < outer)
            onward_dev = jnp.where(exists, onward, mate) * TP + inner
            remote(block, block, onward_dev, number, exists)
        if not (i == 1 and h == 0):
            for dev in ("xy", "yx")[h]:
                copies[dev, i, h] = same(i, "own", chunk[h], dev)
        share(i, "own", h)

    def relay(i, h):
        who, dev = ("x", "y") if h == 0 else ("y", "x")
        if i == 1:
            copies[who, 1, 1].wait_recv()
            copies["d", 1, h] = same(1, who, small_chunk[h], dev)
            share(1, who, 1)
        else:
            copies[who, i, h].wait_recv()
            copies["d", i, h] = same(i, who, chunk[h], dev)
            share(i, who, h)
            if i == 0 and h == 0:
                up_to_mate(0, "x")

    def take(i, h):
        who = "xy"[h]
        copies[who, i, 1 - h].wait_recv()
        share(i, who, 1 - h)
        if i == 0 and h == 1:
            up_to_mate(1, "y")

    def corner(i, h):
        copies["d", i, h].wait_recv()
        if i == 1:
            share(1, "d", 1, small_chunk[h])
        else:
            share(i, "d", h)
            if i == 0 and h == 0:
                up_to_mate(2, "d")

    def from_mate(k):
        copies["m", k].wait_recv()
        share(1, "xyd"[k], 0)

    def weights_over(k):
        begin = k * (units // 2)
        part = pl.ds(begin, units // 2)
        copies["w", k] = remote(
            down.at[0, part, sib_half], w_out.at[pl.ds(units + begin, units // 2)], devs["c"]
        )

    once = set()

    def first(name):
        if name in once:
            return False
        once.add(name)
        return True

    def up(i, h):
        for copy in to_core[i, h]:
            copy.wait_recv()
        if first("in"):
            in_copy.wait()
        o = near[i]
        both = jnp.zeros((rows, 2 * hidden_cols), F32) if h == 0 else acc[i]
        for at, n in spans(0, cut, 512) if h == 0 else spans(cut, width, 512):
            value = xin[o, :, :, pl.ds(at, n)].astype(F32).reshape(rows, n).astype(BF16)
            both = both + jnp.dot(value, w_in[at : at + n, :], preferred_element_type=F32)
        if h == 0:
            acc[i] = both
            return
        hid[i] = (jax.nn.silu(both[:, :hidden_cols]) * both[:, hidden_cols:]).astype(BF16)
        copies["h", i] = remote(hid.at[i], hid_sib.at[i], devs["c"])
        terms = xin[o, :, :, pl.ds(width, LANES)].astype(F32).reshape(rows, LANES)
        lane = lax.broadcasted_iota(jnp.int32, terms.shape, 1)
        keep = (lane % outer == plane) & (lane < 3 * outer)
        gate = jnp.sum(jnp.where(keep, terms, 0.0), axis=1, keepdims=True)
        weight[i] = jnp.broadcast_to(gate, (rows, LANES))

    def mix(i, begin, end, part, x_major, extra=None):
        gate = weight[i][:, :1]
        value_in = jnp.concatenate([hid[i], hid_sib[i]], axis=1)
        for at, n in spans(begin, end, 256):
            value = (
                jnp.dot(value_in, w_out[:, at : at + n], preferred_element_type=F32) * gate
            )
            cols = pl.ds(at - begin, n)
            for s in range(TP):
                sx, sy, sc = s % 2, s // 2 % 2, s // 4
                where = (sx, sy, sc) if x_major else (sy, sx, sc)
                piece = value[s * tok_rows : (s + 1) * tok_rows]
                if extra is not None:
                    piece = piece + extra[(*where, slice(None), cols)].astype(F32)
                part[(*where, slice(None), cols)] = piece.astype(BF16)

    def buffers(i, h):
        at = i if i == 0 else i - 1
        if i == 1:
            return (
                (c_part, c_one, c_mid, c_two, a_cols, g_cols)
                if h == 0
                else (d_part, d_one, d_mid, d_two, g_cols, half)
            )
        if h == 0:
            return a_part.at[i], a_one.at[at], a_mid.at[at], a_two.at[at], 0, a_cols
        return b_part.at[at], b_one.at[at], b_mid.at[at], b_two.at[at], a_cols, half

    def down_part(i, h):
        if first("out"):
            down_copy.wait()
            copies["w", 0].wait_recv()
            copies["w", 1].wait_recv()
        if h == 0:
            copies["h", i].wait_recv()
        if i == 1 and h == 0:
            mix(1, 0, a_cols, a_part.at[1], True)
            copies["f"] = remote(a_part.at[1], f_in, mate_dev)
            return
        extra = None
        if i == 0 and h == 0:
            copies["f"].wait_recv()
            extra = f_in
        for k in (0, 1) if i == 1 else (h,):
            part, one, _, _, begin, end = buffers(i, k)
            mix(i, begin, end, part, k == 0, extra)
            far = 1 - x if k == 0 else 1 - y
            copies["one", i, k] = remote(part.at[far], one, devs["xy"[k]])

    def fold(i, h):
        part, one, middle, two, _, _ = buffers(i, h)
        copies["one", i, h].wait_recv()
        own = x if h == 0 else y
        middle[...] = (part[own].astype(F32) + one[...].astype(F32)).astype(BF16)
        far = 1 - y if h == 0 else 1 - x
        copies["two", i, h] = remote(middle.at[far], two, devs["yx"[h]])

    def finish(i, h):
        _, _, middle, two, begin, end = buffers(i, h)
        copies["two", i, h].wait_recv()
        own = y if h == 0 else x
        cols = pl.ds(begin, end - begin)
        z_send[i, :, :, cols] = (middle[own].astype(F32) + two[...].astype(F32)).astype(BF16)
        landing = z_recv.at[plane, core, :, cols]
        if i == 0:
            copies["fin", h] = remote(z_send.at[0, 1 - core, :, cols], landing, devs["c"])
            return
        side = near[i] * TP + y * 4 + x * 2
        for c in range(2):
            remote(z_send.at[i, c, :, cols], landing, side + c, result_sem(plane, core, h))

    def final():
        for h in range(2):
            copies["fin", h].wait_recv()
        for i in range(1, outer):
            for c in range(2):
                for h in range(2):
                    begin, stop = buffers(i, h)[4:]
                    cols = pl.ds(begin, stop - begin)
                    arrived(z_recv.at[near[i], c, :, cols], result_sem(near[i], c, h))
        z_recv[plane, core] = z_send[0, core]
        for c in range(2):
            for at, n in spans(0, a_cols, 512) + spans(a_cols, half, 512):
                cols = pl.ds(at, n)
                total = z_recv[plane, c, :, cols].astype(F32)
                for i in range(1, outer):
                    if i == 1 and at < a_cols:
                        continue
                    total = total + z_recv[near[i], c, :, cols].astype(F32)
                out[:, c * half + at : c * half + at + n] = total.astype(BF16)

    stages = {
        "A": spread,
        "B": relay,
        "E": take,
        "C": corner,
        "M": from_mate,
        "W": lambda _, k: weights_over(k),
        "D": up,
        "P": down_part,
        "R": fold,
        "S": finish,
    }
    for name in schedule:
        stages[name[0]](*(int(digit) for digit in name[1:]))
    final()
    for copy, when in sent:
        if when is None:
            copy.wait_send()
        else:
            pl.when(when)(copy.wait_send)


PLAN = (
    "A00", "A01", "W00", "W01", "B00", "A11", "A20", "A10",
    "A21", "E01", "B10", "E00", "B01", "C00", "B11", "B20",
    "M0", "B21", "A30", "A31", "M2", "C11", "M1", "C01",
    "C10", "C21", "D00", "E20", "C20", "E21", "D10", "B30",
    "D11", "B31", "D20", "D21", "P10", "P11", "P20", "P21",
    "C30", "E30", "E31", "C31", "D30", "D31", "R10", "D01",
    "R11", "P30", "R20", "R21", "P31", "S10", "S20", "S11",
    "R30", "P00", "P01", "S21", "S30", "R31", "R00", "R01",
    "S31", "S00", "S01",
)


def plan(outer):
    if 2 * outer == 8:
        return PLAN
    when = {"W00": 1.35, "W01": 2.0, "M0": 5.0, "M1": 6.0, "M2": 8.0}
    after = {"A": 0.0, "B": 2.8, "E": 4.0, "C": 5.5, "D": 8.0, "P": 9.0, "R": 13.0, "S": 16.0}
    for i in range(outer):
        begin = 2.7 * i if i < 2 else 4.0 * i - 2.5
        for name, delay in after.items():
            late = 4.0 * outer - 8.0 if i == 0 and name in "PRS" else 0.0
            for h in range(2):
                if (name, i) == ("E", 1):
                    continue
                step = 1.3 if name in "AEC" else 0.4 if name == "B" else 0.2
                when[f"{name}{i}{h}"] = begin + delay + late + step * h
    return tuple(sorted(when, key=when.get))


def local(tokens, route_slot, gates, gate_up, down):
    tok_rows, width = tokens.shape
    outer = lax.axis_size("ea") // TP
    cut, quarter, half, a_cols, g_cols = split(width)
    b_cols, c_cols, d_cols = half - a_cols, g_cols - a_cols, half - g_cols
    rows = TP * tok_rows
    units = down.shape[1]
    buf = lambda *shape: pltpu.VMEM(shape, BF16)
    copies = copies_per_launch(outer)
    parts = [buf(2, 2, 2, tok_rows, n) for n in (c_cols, d_cols)]
    full = outer - 1
    widths = (a_cols, b_cols)
    scratch = [
        buf(outer, TP, tok_rows, width + LANES),
        pltpu.VMEM((outer, rows, gate_up.shape[2]), F32),
        buf(outer, rows, units),
        buf(outer, rows, units),
        pltpu.VMEM((outer, rows, LANES), F32),
        pltpu.VMEM(gate_up.shape[1:], BF16),
        buf(2 * units, half),
        buf(outer, 2, 2, 2, tok_rows, a_cols),
        buf(full, 2, 2, 2, tok_rows, b_cols),
        *parts,
        buf(2, 2, 2, tok_rows, a_cols),
        *[buf(full, 2, 2, tok_rows, n) for n in widths],
        *[buf(2, 2, tok_rows, n) for n in (c_cols, d_cols)],
        *[buf(full, 2, 2, tok_rows, n) for n in widths],
        *[buf(2, 2, tok_rows, n) for n in (c_cols, d_cols)],
        *[buf(full, 2, tok_rows, n) for n in widths],
        *[buf(2, tok_rows, n) for n in (c_cols, d_cols)],
        buf(outer, 2, tok_rows, half),
        buf(outer, 2, tok_rows, half),
        pltpu.VMEM(route_slot.shape[::-1], route_slot.dtype),
        pltpu.VMEM(gates.shape[::-1], gates.dtype),
        pltpu.SemaphoreType.DMA((copies,)),
        pltpu.SemaphoreType.DMA((copies + 6 * outer,)),
        pltpu.SemaphoreType.DMA((5,)),
    ]
    vmem = pl.BlockSpec(memory_space=pltpu.VMEM)
    hbm = pl.BlockSpec(memory_space=pl.ANY)
    return pl.pallas_call(
        functools.partial(kernel, outer, plan(outer)),
        out_shape=jax.ShapeDtypeStruct((tok_rows, width), BF16),
        in_specs=[hbm] * 5,
        out_specs=vmem,
        scratch_shapes=scratch,
        compiler_params=pltpu.CompilerParams(
            collective_id=0, has_side_effects=True, vmem_limit_bytes=60000 * 1024
        ),
    )(tokens, route_slot.T, gates.T, gate_up, down)


def solution(mesh):
    placed = (
        P(("ga", "ea"), None),
        P(("ga", "ea"), None),
        P(("ga", "ea"), None),
        P("ea", None, None),
        P("ea", None, None),
    )
    return jax.shard_map(
        local, mesh=mesh, in_specs=placed, out_specs=P(("ga", "ea"), None), check_vma=False
    )
```
